32 devices in a mesh: expert: 8 (over z, x), pair: 4 (over y, core).
Axes of the slice: x: 2, y: 2, z: 4, core: 2. Of those that a mesh axis runs over, the one named last changes fastest.
Arguments:
- tokens: bfloat16 [12288, 2048], P(('expert', 'pair')), may hold values from -6 to 6
- token_ids: int32 [12288], P(('expert', 'pair')), may hold values from 0 to 8191
- table: int32 [8192], replicated, may hold values from 0 to 15
- w_in: bfloat16 [16, 2048, 2048], P('expert', None, 'pair'), may hold values from -0.125 to 0.125
- w_out: bfloat16 [16, 2048, 2048], P('expert', 'pair'), may hold values from -0.125 to 0.125
Outputs:
- mixed: bfloat16 [12288, 2048], P(('expert', 'pair'))
The draws below stay inside these ranges and needn't reach their ends.
All inputs are finite; a program needn't handle non-finite values.
Results may differ from the reference program's by a relative error of at most 0.0085.
Values may be sent and summed in bfloat16 or wider, within the bound.
A program may use at most 192 MiB of HBM per device.

```python
import math
import jax
import jax.numpy as jnp
import numpy as np
from jax import lax

D = 2048
H = 2048
VOCAB = 8192
TOK_DEV = 384
EXPERTS = 16
CAP = 48
TOKENS = 12288
N_EXPERT = 8
N_PAIR = 4


def touch_ends(result, stream_key, smallest, high):
    index_at = [jax.random.randint(jax.random.fold_in(stream_key, axis), (), 0, length) for axis, length in enumerate(result.shape)]
    longest = result.shape.index(max(result.shape))
    beside = index_at[:longest] + [(index_at[longest] + 1) % result.shape[longest]] + index_at[longest + 1:]
    return result.at[tuple(index_at)].set(smallest).at[tuple(beside)].set(high)


def level_of(key, dims, pieces, low, largest):
    def one(dim, shards_of):
        draws = jax.random.uniform(jax.random.fold_in(jax.random.fold_in(key, 6), dim), (shards_of,), jnp.float32, low / len(pieces), largest / len(pieces))
        return jnp.repeat(jnp.exp(draws), dims[dim] // shards_of).reshape((-1,) + (1,) * (len(dims) - dim - 1))

    gain = one(*pieces[0])
    for cut in pieces[1:]:
        gain = gain * one(*cut)
    return gain


def cumulative_ranks(number_of, lean):
    portions = [(1 << 20) // math.isqrt(grade ** lean) + 1 for grade in range(1, number_of + 1)]
    width = 1 + sum(portions) // (1 << 30)
    return np.cumsum(np.array([max(1, weight // width) for weight in portions]))


def ranked(rng, extent, amount, slope):
    table = cumulative_ranks(amount, slope)
    ticket = jax.random.randint(jax.random.fold_in(rng, 1), extent, 0, int(table[amount - 1]))
    grade = jnp.searchsorted(jnp.asarray(table, jnp.int32), ticket, side="right")
    return jax.random.permutation(jax.random.fold_in(rng, 2), amount)[grade].astype(jnp.int32)


def scatter_about(key, shape, width, reach, pieces=(), kind=jnp.bfloat16):
    array = jax.random.normal(key, shape, jnp.float32) * width
    if len(pieces) > 0:
        array = level_of(key, shape, pieces, -0.22, 0.18) * array
    return jnp.clip(array, min=-reach, max=reach).astype(kind)


def setup_inputs(seed: int = 0) -> dict:
    arg_keys = jax.random.split(jax.random.key(seed), 6)
    tokens = scatter_about(arg_keys[0], (TOKENS, D), 1.0, 6.0, ((0, 32),))
    token_ids = touch_ends(ranked(arg_keys[1], (TOKENS,), VOCAB, 2), jax.random.fold_in(arg_keys[1], 3), 0, VOCAB - 1).astype(jnp.int32)
    table = touch_ends(jax.random.randint(arg_keys[2], (VOCAB,), 0, EXPERTS), jax.random.fold_in(arg_keys[2], 1), 0, EXPERTS - 1).astype(jnp.int32)
    w_in = scatter_about(arg_keys[3], (EXPERTS, D, H), D ** -0.5, 0.125, ((0, 8), (2, 4)))
    w_out = scatter_about(arg_keys[4], (EXPERTS, H, D), H ** -0.5, 0.125, ((0, 8), (1, 4)))
    return {"tokens": tokens, "token_ids": token_ids, "table": table, "w_in": w_in, "w_out": w_out}


def reference(tokens, token_ids, table, w_in, w_out):
    blocks = N_EXPERT * N_PAIR
    quarter = H // N_PAIR
    chosen = jnp.take(table, token_ids, axis=0).astype(jnp.int32).reshape(blocks, TOK_DEV)
    hot = (chosen[:, :, None] == jnp.arange(EXPERTS, dtype=jnp.int32)[None, None, :]).astype(jnp.int32)
    earlier = jnp.cumsum(hot, axis=1) - hot
    rank = jnp.sum(earlier * hot, axis=2)
    kept = rank < CAP
    block_index = jnp.arange(blocks, dtype=jnp.int32)[:, None]
    total_slots = EXPERTS * blocks * CAP
    position = (chosen * blocks + block_index) * CAP + rank
    position = jnp.where(kept, position, total_slots).reshape(-1).astype(jnp.int32)
    buffer = jnp.zeros((total_slots, D), jnp.bfloat16).at[position].set(tokens, mode="drop")
    buffer = buffer.reshape(EXPERTS, blocks * CAP, D)

    def one_expert(items):
        rows, first, second = items
        hidden = jax.nn.relu(jnp.dot(rows, first, preferred_element_type=jnp.float32)).astype(jnp.bfloat16)
        total = jnp.zeros((rows.shape[0], D), jnp.float32)
        for index in range(N_PAIR):
            part = jnp.dot(hidden[:, index * quarter:(index + 1) * quarter],
                           second[index * quarter:(index + 1) * quarter],
                           preferred_element_type=jnp.float32).astype(jnp.bfloat16)
            total = total + lax.optimization_barrier(part).astype(jnp.float32)
        return total.astype(jnp.bfloat16)

    outputs = lax.map(one_expert, (buffer, w_in, w_out)).reshape(total_slots, D)
    safe = jnp.minimum(position, total_slots - 1).astype(jnp.int32)
    picked = jnp.take(outputs, safe, axis=0)
    mixed = jnp.where(kept.reshape(-1)[:, None], picked, jnp.zeros_like(picked))
    return mixed.astype(jnp.bfloat16)
```

```python
import functools

import jax
import jax.numpy as jnp
from jax import lax
from jax.experimental import pallas as pl
from jax.experimental.pallas import tpu as pltpu
from jax.sharding import PartitionSpec as P

ROWS = 16
TILE = 256
MESH = pl.DeviceIdType.MESH


def exact_dot(a, b):
    return jnp.dot(a, b, preferred_element_type=jnp.float32)


def layer_kernel(
    n,
    packed,
    w_in,
    w_out,
    back,
    first,
    second,
    rows,
    hidden,
    part,
    near,
    far,
    own_sem,
    w_sem,
    go_sem,
    come_sem,
    pair_go,
    pair_come,
):
    chunks = packed.shape[0]
    per_expert = chunks // w_in.shape[0]
    me = lax.axis_index("expert")
    at = lax.axis_index("pair")
    core = {"pair": at + 1 - 2 * (at % 2)}
    chip = {"pair": (at + 2) % 4}
    ahead = [{"expert": (me + j) % n} for j in range(n)]
    behind = [{"expert": (me + n - j) % n} for j in range(n)]

    w_copies = [
        pltpu.make_async_copy(w_in, first, w_sem.at[0]),
        pltpu.make_async_copy(w_out, second, w_sem.at[1]),
    ]
    for copy in w_copies:
        copy.start()

    barrier = pltpu.get_barrier_semaphore()
    for peer in [core, chip] + ahead[1:]:
        pl.semaphore_signal(barrier, inc=1, device_id=peer, device_id_type=MESH)
    pl.semaphore_wait(barrier, n + 1)

    def remote(src, dst, send, recv, peer):
        copy = pltpu.make_async_remote_copy(
            src_ref=src,
            dst_ref=dst,
            send_sem=send,
            recv_sem=recv,
            device_id=peer,
            device_id_type=MESH,
        )
        copy.start()
        return copy

    sent = []
    dispatch = []
    for c in range(chunks):
        copies = [
            remote(
                packed.at[c, pl.ds(j * ROWS, ROWS)],
                rows.at[c, 0, pl.ds(j * ROWS, ROWS)],
                go_sem.at[0, c, j],
                come_sem.at[0, c, j],
                ahead[j],
            )
            for j in range(1, n)
        ]
        own = pltpu.make_async_copy(
            packed.at[c, pl.ds(0, ROWS)], rows.at[c, 0, pl.ds(0, ROWS)], own_sem.at[0, c]
        )
        own.start()
        dispatch.append((own, copies))

    links = {}

    def pair_send(kind, c, src, dst, peer):
        links[kind, c] = remote(src, dst, pair_go.at[kind, c], pair_come.at[kind, c], peer)

    def spread(c):
        own, copies = dispatch[c]
        own.wait()
        for copy in copies:
            copy.wait_recv()
        pair_send(0, c, rows.at[c, 0], rows.at[c, 2], chip)
        pair_send(1, c, rows.at[c, 0], rows.at[c, 1], core)

    def relay(c):
        links[0, c].wait_recv()
        pair_send(2, c, rows.at[c, 2], rows.at[c, 3], core)

    def compute(c):
        e = c // per_expert
        if c == 0:
            for copy in w_copies:
                copy.wait()
        links[1, c].wait_recv()
        links[2, c].wait_recv()
        block = rows.shape[2]

        def project_in(t, carry):
            cols = pl.ds(pl.multiple_of(t * TILE, TILE), TILE)
            x = rows[c].reshape(4 * block, rows.shape[3])
            h = exact_dot(x, first[e, :, cols])
            hidden[:, cols] = jnp.maximum(h, 0.0).astype(jnp.bfloat16)
            return carry

        lax.fori_loop(0, first.shape[2] // TILE, project_in, 0)

        def project_out(t, carry):
            cols = pl.ds(pl.multiple_of(t * TILE, TILE), TILE)
            y = exact_dot(hidden[...], second[e, :, cols]).astype(jnp.bfloat16)
            for k in range(4):
                part[c, k, :, cols] = y[k * block : (k + 1) * block]
            return carry

        lax.fori_loop(0, second.shape[2] // TILE, project_out, 0)
        pair_send(3, c, part.at[c, 3], near.at[c, 1], core)
        pair_send(4, c, part.at[c, 1], near.at[c, 0], core)

    def over_rows(body):
        def step(t, carry):
            body(pl.ds(pl.multiple_of(t * ROWS, ROWS), ROWS))
            return carry

        lax.fori_loop(0, n, step, 0)

    def wide(x):
        return x.astype(jnp.float32)

    def cross(c):
        links[3, c].wait_recv()

        def add(r):
            both = wide(part[c, 2, r, :]) + wide(near[c, 1, r, :])
            part[c, 2, r, :] = both.astype(jnp.bfloat16)

        over_rows(add)
        pair_send(5, c, part.at[c, 2], far.at[c], chip)

    def finish(c):
        links[4, c].wait_recv()
        links[5, c].wait_recv()

        def add(r):
            both = wide(part[c, 0, r, :]) + wide(near[c, 0, r, :]) + wide(far[c, r, :])
            part[c, 0, r, :] = both.astype(jnp.bfloat16)

        over_rows(add)
        for j in range(1, n):
            block = pl.ds(j * ROWS, ROWS)
            sent.append(
                remote(
                    part.at[c, 0, block],
                    back.at[c, block],
                    go_sem.at[1, c, j],
                    come_sem.at[1, c, j],
                    behind[j],
                )
            )
        own = pltpu.make_async_copy(
            part.at[c, 0, pl.ds(0, ROWS)], back.at[c, pl.ds(0, ROWS)], own_sem.at[1, c]
        )
        own.start()
        sent.append(own)

    for i in range(chunks + 3):
        if i < chunks:
            spread(i)
        if 0 <= i - 1 < chunks:
            relay(i - 1)
            compute(i - 1)
        if 0 <= i - 2 < chunks:
            cross(i - 2)
        if 0 <= i - 3 < chunks:
            finish(i - 3)

    for _, copies in dispatch:
        for copy in copies:
            copy.wait_send()
    for copy in links.values():
        copy.wait_send()
    for copy in sent:
        copy.wait()


def expert_layer(packed, w_in, w_out, n):
    chunks, block, width = packed.shape
    quarter = w_in.shape[2]
    bf16 = jnp.bfloat16
    dma = pltpu.SemaphoreType.DMA
    anywhere = pl.BlockSpec(memory_space=pl.ANY)
    return pl.pallas_call(
        functools.partial(layer_kernel, n),
        out_shape=jax.ShapeDtypeStruct(packed.shape, bf16),
        in_specs=[anywhere] * 3,
        out_specs=anywhere,
        scratch_shapes=[
            pltpu.VMEM(w_in.shape, bf16),
            pltpu.VMEM(w_out.shape, bf16),
            pltpu.VMEM((chunks, 4, block, width), bf16),
            pltpu.VMEM((4 * block, quarter), bf16),
            pltpu.VMEM((chunks, 4, block, width), bf16),
            pltpu.VMEM((chunks, 2, block, width), bf16),
            pltpu.VMEM((chunks, block, width), bf16),
            dma((2, chunks)),
            dma((2,)),
            dma((2, chunks, n)),
            dma((2, chunks, n)),
            dma((6, chunks)),
            dma((6, chunks)),
        ],
        compiler_params=pltpu.CompilerParams(
            collective_id=0, has_side_effects=True, vmem_limit_bytes=60 * 1024 * 1024
        ),
    )(packed, w_in, w_out)


def plain(tokens, token_ids, table, w_in, w_out):
    groups = lax.axis_size("expert")
    exp_local = w_in.shape[0]
    experts = groups * exp_local
    tok_rows, width = tokens.shape
    slots = max(2, 2 * tok_rows // experts)
    quarter = w_out.shape[1]
    chosen = jnp.take(table, token_ids, axis=0)
    expert_hot = (chosen[:, None] == jnp.arange(experts, dtype=jnp.int32)[None, :]).astype(
        jnp.int32
    )
    earlier = jnp.cumsum(expert_hot, axis=0) - expert_hot
    rank_tok = jnp.sum(earlier * expert_hot, axis=1)
    kept = rank_tok < slots
    column = (chosen // exp_local * slots + rank_tok) * exp_local + chosen % exp_local
    placer = (
        (column[:, None] == jnp.arange(experts * slots, dtype=jnp.int32)[None, :]) & kept[:, None]
    ).astype(jnp.bfloat16)
    packed = jnp.einsum("ts,td->sd", placer, tokens, preferred_element_type=jnp.float32).astype(
        jnp.bfloat16
    )
    packed = packed.reshape(groups * slots, exp_local, width)
    arrived = lax.all_to_all(packed, "expert", split_axis=0, concat_axis=0, tiled=True)
    rows = arrived.shape[0]
    hidden = jax.nn.relu(
        jnp.einsum(
            "red,edh->reh",
            arrived,
            lax.all_gather(w_in, "pair", axis=2, tiled=True),
            preferred_element_type=jnp.float32,
        )
    ).astype(jnp.bfloat16)
    total = jnp.zeros((rows, exp_local, width), jnp.float32)
    piece = lax.all_gather(w_out, "pair", axis=1, tiled=True)
    for index in range(piece.shape[1] // quarter):
        cols = lax.dynamic_slice_in_dim(hidden, index * quarter, quarter, 2)
        part = jnp.einsum(
            "reh,ehd->red",
            cols,
            piece[:, index * quarter : (index + 1) * quarter],
            preferred_element_type=jnp.float32,
        ).astype(jnp.bfloat16)
        total = total + lax.optimization_barrier(part).astype(jnp.float32)
    result = total.astype(jnp.bfloat16)
    returned = lax.all_to_all(result, "expert", split_axis=0, concat_axis=0, tiled=True)
    flat = returned.reshape(experts * slots, width)
    return jnp.dot(placer, flat, preferred_element_type=jnp.float32).astype(jnp.bfloat16)


def on_device(tokens, token_ids, table, w_in, w_out):
    n = lax.axis_size("expert")
    me = lax.axis_index("expert")
    exp_local = w_in.shape[0]
    experts = n * exp_local
    tok_rows, width = tokens.shape
    slots = max(2, 2 * tok_rows // experts)
    if slots % ROWS or lax.axis_size("pair") != 4:
        return plain(tokens, token_ids, table, w_in, w_out)
    per_expert = slots // ROWS

    chosen = jnp.take(table, token_ids, axis=0)
    hot = chosen[:, None] == jnp.arange(experts, dtype=jnp.int32)[None, :]
    before = jnp.arange(tok_rows)[:, None] > jnp.arange(tok_rows)[None, :]
    earlier = exact_dot(before.astype(jnp.bfloat16), hot.astype(jnp.bfloat16))
    rank = jnp.sum(jnp.where(hot, earlier, 0.0), axis=1).astype(jnp.int32)
    ahead = (chosen // exp_local - me + n) % n
    chunk = chosen % exp_local * per_expert + rank // ROWS
    column = jnp.where(rank < slots, (chunk * n + ahead) * ROWS + rank % ROWS, -1)

    places = jnp.arange(experts * slots, dtype=jnp.int32)
    placer = (places[:, None] == column[None, :]).astype(jnp.bfloat16)
    packed = exact_dot(placer, tokens).astype(jnp.bfloat16)
    packed = packed.reshape(exp_local * per_expert, n * ROWS, width)
    back = expert_layer(packed, w_in, w_out, n).reshape(experts * slots, width)
    picker = (column[:, None] == places[None, :]).astype(jnp.bfloat16)
    return exact_dot(picker, back).astype(jnp.bfloat16)


def solution(mesh):
    in_specs = (
        P(("expert", "pair"), None),
        P(("expert", "pair")),
        P(),
        P("expert", None, "pair"),
        P("expert", "pair", None),
    )
    out_specs = P(("expert", "pair"), None)
    return jax.shard_map(
        on_device, mesh=mesh, in_specs=in_specs, out_specs=out_specs, check_vma=False
    )
```

```python
import functools

import jax
import jax.numpy as jnp
from jax import lax
from jax.experimental import pallas as pl
from jax.experimental.pallas import tpu as pltpu
from jax.sharding import PartitionSpec as P

ROWS = 16
TILE = 256
LAST_PIECES = 4
LANES = 128
MESH = pl.DeviceIdType.MESH


def exact_dot(a, b):
    return jnp.dot(a, b, preferred_element_type=jnp.float32)


def layer_kernel(
    n,
    packed,
    w_in,
    w_out,
    back,
    first,
    second,
    rows,
    hidden,
    part,
    near,
    far,
    own_sem,
    w_sem,
    go_sem,
    come_sem,
    pair_go,
    pair_come,
    part_go,
    part_come,
    ret_go,
    ret_come,
    ret_own,
):
    chunks = packed.shape[0]
    per_expert = chunks // w_in.shape[0]
    me = lax.axis_index("expert")
    at = lax.axis_index("pair")
    core = {"pair": at + 1 - 2 * (at % 2)}
    chip = {"pair": (at + 2) % 4}
    ahead = [{"expert": (me + j) % n} for j in range(n)]
    behind = [{"expert": (me + n - j) % n} for j in range(n)]

    w_copies = [
        pltpu.make_async_copy(w_in, first, w_sem.at[0]),
        pltpu.make_async_copy(w_out, second, w_sem.at[1]),
    ]
    for copy in w_copies:
        copy.start()

    barrier = pltpu.get_barrier_semaphore()
    for peer in [core, chip] + ahead[1:]:
        pl.semaphore_signal(barrier, inc=1, device_id=peer, device_id_type=MESH)
    pl.semaphore_wait(barrier, n + 1)

    def remote(src, dst, send, recv, peer):
        copy = pltpu.make_async_remote_copy(
            src_ref=src,
            dst_ref=dst,
            send_sem=send,
            recv_sem=recv,
            device_id=peer,
            device_id_type=MESH,
        )
        copy.start()
        return copy

    sent = []
    dispatch = []
    links = {}

    def pair_send(kind, c, src, dst, peer):
        links[kind, c] = remote(src, dst, pair_go.at[kind, c], pair_come.at[kind, c], peer)

    def blocks(lo, hi):
        return pl.ds(lo * ROWS, (hi - lo) * ROWS)

    for c in range(chunks):
        dispatch.append(
            [
                remote(
                    packed.at[c, blocks(j, j + 1)],
                    rows.at[c, 0, blocks(j, j + 1)],
                    go_sem.at[c, j],
                    come_sem.at[c, j],
                    ahead[j],
                )
                for j in range(1, n)
            ]
        )
    own_copies = []
    for c in range(chunks):
        own = blocks(0, 1)
        pair_send(0, c, packed.at[c, own], rows.at[c, 2, own], chip)
        pair_send(1, c, packed.at[c, own], rows.at[c, 1, own], core)
        copy = pltpu.make_async_copy(packed.at[c, own], rows.at[c, 0, own], own_sem.at[c])
        copy.start()
        own_copies.append(copy)

    groups = [(1, n // 2), (n // 2, n)]

    def spread(c):
        for g, (lo, hi) in enumerate(groups):
            for j in range(lo, hi):
                dispatch[c][j - 1].wait_recv()
            some = blocks(lo, hi)
            pair_send(2 + 2 * g, c, rows.at[c, 0, some], rows.at[c, 2, some], chip)
            pair_send(3 + 2 * g, c, rows.at[c, 0, some], rows.at[c, 1, some], core)

    def relay(c):
        for kind in (0, 2, 4):
            links[kind, c].wait_recv()
        pair_send(6, c, rows.at[c, 2], rows.at[c, 3], core)

    def pieces(c):
        return LAST_PIECES if c == chunks - 1 else 1

    def columns(c, q):
        size = part.shape[3] // pieces(c)
        return pl.ds(q * size, size)

    def part_send(kind, c, q, src, dst, peer):
        links[kind, c, q] = remote(
            src, dst, part_go.at[kind, c, q], part_come.at[kind, c, q], peer
        )

    def compute(c):
        e = c // per_expert
        if c == 0:
            for copy in w_copies:
                copy.wait()
        own_copies[c].wait()
        for kind in (1, 3, 5, 6):
            links[kind, c].wait_recv()
        block = rows.shape[2]

        def project_in(t, carry):
            cols = pl.ds(pl.multiple_of(t * TILE, TILE), TILE)
            x = rows[c].reshape(4 * block, rows.shape[3])
            h = exact_dot(x, first[e, :, cols])
            hidden[:, cols] = jnp.maximum(h, 0.0).astype(jnp.bfloat16)
            return carry

        lax.fori_loop(0, first.shape[2] // TILE, project_in, 0)

        def project_out(t, carry):
            cols = pl.ds(pl.multiple_of(t * TILE, TILE), TILE)
            y = exact_dot(hidden[...], second[e, :, cols]).astype(jnp.bfloat16)
            for k in range(4):
                part[c, k, :, cols] = y[k * block : (k + 1) * block]
            return carry

        steps = second.shape[2] // TILE // pieces(c)
        for q in range(pieces(c)):
            lax.fori_loop(q * steps, (q + 1) * steps, project_out, 0)
            cols = columns(c, q)
            part_send(0, c, q, part.at[c, 3, :, cols], near.at[c, 1, :, cols], core)
            part_send(1, c, q, part.at[c, 1, :, cols], near.at[c, 0, :, cols], core)

    def over_rows(body):
        def step(t, carry):
            body(pl.ds(pl.multiple_of(t * ROWS, ROWS), ROWS))
            return carry

        lax.fori_loop(0, n, step, 0)

    def wide(x):
        return x.astype(jnp.float32)

    def cross(c):
        for q in range(pieces(c)):
            links[0, c, q].wait_recv()
            cols = columns(c, q)

            def add(r):
                both = wide(part[c, 2, r, cols]) + wide(near[c, 1, r, cols])
                part[c, 2, r, cols] = both.astype(jnp.bfloat16)

            over_rows(add)
            part_send(2, c, q, part.at[c, 2, :, cols], far.at[c, :, cols], chip)

    def finish(c):
        for q in range(pieces(c)):
            links[1, c, q].wait_recv()
            links[2, c, q].wait_recv()
            cols = columns(c, q)

            def add(r):
                both = wide(part[c, 0, r, cols]) + wide(near[c, 0, r, cols])
                both = both + wide(far[c, r, cols])
                part[c, 0, r, cols] = both.astype(jnp.bfloat16)

            over_rows(add)
            for j in range(1, n):
                some = blocks(j, j + 1)
                sent.append(
                    remote(
                        part.at[c, 0, some, cols],
                        back.at[c, some, cols],
                        ret_go.at[c, q, j],
                        ret_come.at[c, q, j],
                        behind[j],
                    )
                )
            own = blocks(0, 1)
            copy = pltpu.make_async_copy(
                part.at[c, 0, own, cols], back.at[c, own, cols], ret_own.at[c, q]
            )
            copy.start()
            sent.append(copy)

    for i in range(chunks + 3):
        if i < chunks:
            spread(i)
        if 0 <= i - 1 < chunks:
            relay(i - 1)
            compute(i - 1)
        if 0 <= i - 2 < chunks:
            cross(i - 2)
        if 0 <= i - 3 < chunks:
            finish(i - 3)

    for copies in dispatch:
        for copy in copies:
            copy.wait_send()
    for copy in links.values():
        copy.wait_send()
    for copy in sent:
        copy.wait()


def look_up(table, ids):
    lines = table.reshape(-1, LANES).astype(jnp.bfloat16)
    line = ids[:, None] // LANES == jnp.arange(lines.shape[0], dtype=jnp.int32)[None, :]
    found = exact_dot(line.astype(jnp.bfloat16), lines)
    lane = ids[:, None] % LANES == jnp.arange(LANES, dtype=jnp.int32)[None, :]
    return jnp.sum(jnp.where(lane, found, 0.0), axis=1).astype(jnp.int32)


def expert_layer(packed, w_in, w_out, n):
    chunks, block, width = packed.shape
    quarter = w_in.shape[2]
    bf16 = jnp.bfloat16
    dma = pltpu.SemaphoreType.DMA
    anywhere = pl.BlockSpec(memory_space=pl.ANY)
    return pl.pallas_call(
        functools.partial(layer_kernel, n),
        out_shape=jax.ShapeDtypeStruct(packed.shape, bf16),
        in_specs=[anywhere] * 3,
        out_specs=anywhere,
        scratch_shapes=[
            pltpu.VMEM(w_in.shape, bf16),
            pltpu.VMEM(w_out.shape, bf16),
            pltpu.VMEM((chunks, 4, block, width), bf16),
            pltpu.VMEM((4 * block, quarter), bf16),
            pltpu.VMEM((chunks, 4, block, width), bf16),
            pltpu.VMEM((chunks, 2, block, width), bf16),
            pltpu.VMEM((chunks, block, width), bf16),
            dma((chunks,)),
            dma((2,)),
            dma((chunks, n)),
            dma((chunks, n)),
            dma((7, chunks)),
            dma((7, chunks)),
            dma((3, chunks, LAST_PIECES)),
            dma((3, chunks, LAST_PIECES)),
            dma((chunks, LAST_PIECES, n)),
            dma((chunks, LAST_PIECES, n)),
            dma((chunks, LAST_PIECES)),
        ],
        compiler_params=pltpu.CompilerParams(
            collective_id=0, has_side_effects=True, vmem_limit_bytes=60 * 1024 * 1024
        ),
    )(packed, w_in, w_out)


def plain(tokens, token_ids, table, w_in, w_out):
    groups = lax.axis_size("expert")
    exp_local = w_in.shape[0]
    experts = groups * exp_local
    tok_rows, width = tokens.shape
    slots = max(2, 2 * tok_rows // experts)
    quarter = w_out.shape[1]
    chosen = jnp.take(table, token_ids, axis=0)
    expert_hot = (chosen[:, None] == jnp.arange(experts, dtype=jnp.int32)[None, :]).astype(
        jnp.int32
    )
    earlier = jnp.cumsum(expert_hot, axis=0) - expert_hot
    rank_tok = jnp.sum(earlier * expert_hot, axis=1)
    kept = rank_tok < slots
    column = (chosen // exp_local * slots + rank_tok) * exp_local + chosen % exp_local
    placer = (
        (column[:, None] == jnp.arange(experts * slots, dtype=jnp.int32)[None, :]) & kept[:, None]
    ).astype(jnp.bfloat16)
    packed = jnp.einsum("ts,td->sd", placer, tokens, preferred_element_type=jnp.float32).astype(
        jnp.bfloat16
    )
    packed = packed.reshape(groups * slots, exp_local, width)
    arrived = lax.all_to_all(packed, "expert", split_axis=0, concat_axis=0, tiled=True)
    rows = arrived.shape[0]
    hidden = jax.nn.relu(
        jnp.einsum(
            "red,edh->reh",
            arrived,
            lax.all_gather(w_in, "pair", axis=2, tiled=True),
            preferred_element_type=jnp.float32,
        )
    ).astype(jnp.bfloat16)
    total = jnp.zeros((rows, exp_local, width), jnp.float32)
    piece = lax.all_gather(w_out, "pair", axis=1, tiled=True)
    for index in range(piece.shape[1] // quarter):
        cols = lax.dynamic_slice_in_dim(hidden, index * quarter, quarter, 2)
        part = jnp.einsum(
            "reh,ehd->red",
            cols,
            piece[:, index * quarter : (index + 1) * quarter],
            preferred_element_type=jnp.float32,
        ).astype(jnp.bfloat16)
        total = total + lax.optimization_barrier(part).astype(jnp.float32)
    result = total.astype(jnp.bfloat16)
    returned = lax.all_to_all(result, "expert", split_axis=0, concat_axis=0, tiled=True)
    flat = returned.reshape(experts * slots, width)
    return jnp.dot(placer, flat, preferred_element_type=jnp.float32).astype(jnp.bfloat16)


def on_device(tokens, token_ids, table, w_in, w_out):
    n = lax.axis_size("expert")
    me = lax.axis_index("expert")
    exp_local = w_in.shape[0]
    experts = n * exp_local
    tok_rows, width = tokens.shape
    slots = max(2, 2 * tok_rows // experts)
    if slots % ROWS or table.shape[0] % LANES or lax.axis_size("pair") != 4 or experts > 256:
        return plain(tokens, token_ids, table, w_in, w_out)
    per_expert = slots // ROWS

    chosen = look_up(table, token_ids)
    hot = chosen[:, None] == jnp.arange(experts, dtype=jnp.int32)[None, :]
    before = jnp.arange(tok_rows)[:, None] > jnp.arange(tok_rows)[None, :]
    earlier = exact_dot(before.astype(jnp.bfloat16), hot.astype(jnp.bfloat16))
    rank = jnp.sum(jnp.where(hot, earlier, 0.0), axis=1).astype(jnp.int32)
    ahead = (chosen // exp_local - me + n) % n
    chunk = chosen % exp_local * per_expert + rank // ROWS
    column = jnp.where(rank < slots, (chunk * n + ahead) * ROWS + rank % ROWS, -1)

    places = jnp.arange(experts * slots, dtype=jnp.int32)
    placer = (places[:, None] == column[None, :]).astype(jnp.bfloat16)
    packed = exact_dot(placer, tokens).astype(jnp.bfloat16)
    packed = packed.reshape(exp_local * per_expert, n * ROWS, width)
    back = expert_layer(packed, w_in, w_out, n).reshape(experts * slots, width)
    picker = (column[:, None] == places[None, :]).astype(jnp.bfloat16)
    return exact_dot(picker, back).astype(jnp.bfloat16)


def solution(mesh):
    in_specs = (
        P(("expert", "pair"), None),
        P(("expert", "pair")),
        P(),
        P("expert", None, "pair"),
        P("expert", "pair", None),
    )
    out_specs = P(("expert", "pair"), None)
    return jax.shard_map(
        on_device, mesh=mesh, in_specs=in_specs, out_specs=out_specs, check_vma=False
    )
```

```python
import functools

import jax
import jax.numpy as jnp
from jax import lax
from jax.experimental import pallas as pl
from jax.experimental.pallas import tpu as pltpu
from jax.sharding import PartitionSpec as P

ROWS = 16
TILE = 256
LAST_PIECES = 4
LANES = 128
MESH = pl.DeviceIdType.MESH


def exact_dot(a, b):
    return jnp.dot(a, b, preferred_element_type=jnp.float32)


def across(me, j):
    other = me
    bit = 1
    while bit <= j:
        if j & bit:
            other = other + bit * (1 - 2 * (me // bit % 2))
        bit *= 2
    return other


def send_order(chunks, n):
    first = [(c, 1) for c in range(chunks)]
    return first + [(c, j) for c in range(chunks) for j in range(2, n)]


def layer_kernel(
    n,
    packed,
    w_in,
    w_out,
    back,
    first,
    second,
    rows,
    hidden,
    part,
    near,
    far,
    own_sem,
    w_sem,
    go_sem,
    come_sem,
    pair_go,
    pair_come,
    part_go,
    part_come,
    ret_go,
    ret_come,
    ret_own,
):
    chunks = packed.shape[0]
    per_expert = chunks // w_in.shape[0]
    me = lax.axis_index("expert")
    at = lax.axis_index("pair")
    core = {"pair": at + 1 - 2 * (at % 2)}
    chip = {"pair": (at + 2) % 4}
    ahead = [{"expert": across(me, j)} for j in range(n)]

    w_copies = [
        pltpu.make_async_copy(w_in, first, w_sem.at[0]),
        pltpu.make_async_copy(w_out, second, w_sem.at[1]),
    ]
    for copy in w_copies:
        copy.start()

    barrier = pltpu.get_barrier_semaphore()
    for peer in [core, chip] + ahead[1:]:
        pl.semaphore_signal(barrier, inc=1, device_id=peer, device_id_type=MESH)
    pl.semaphore_wait(barrier, n + 1)

    def remote(src, dst, send, recv, peer):
        copy = pltpu.make_async_remote_copy(
            src_ref=src,
            dst_ref=dst,
            send_sem=send,
            recv_sem=recv,
            device_id=peer,
            device_id_type=MESH,
        )
        copy.start()
        return copy

    sent = []
    dispatch = {}
    links = {}

    def pair_send(kind, c, src, dst, peer):
        links[kind, c] = remote(src, dst, pair_go.at[kind, c], pair_come.at[kind, c], peer)

    def blocks(lo, hi):
        return pl.ds(lo * ROWS, (hi - lo) * ROWS)

    def send_block(c, j):
        dispatch[c, j] = remote(
            packed.at[c, blocks(j, j + 1)],
            rows.at[c, 0, blocks(j, j + 1)],
            go_sem.at[c, j],
            come_sem.at[c, j],
            ahead[j],
        )

    for c, j in send_order(chunks, n):
        send_block(c, j)
    own_copies = []
    for c in range(chunks):
        own = blocks(0, 1)
        pair_send(0, c, packed.at[c, own], rows.at[c, 2, own], chip)
        pair_send(1, c, packed.at[c, own], rows.at[c, 1, own], core)
        copy = pltpu.make_async_copy(packed.at[c, own], rows.at[c, 0, own], own_sem.at[c])
        copy.start()
        own_copies.append(copy)

    groups = [(1, 2), (2, n // 2), (n // 2, n)]

    def spread(c, g):
        lo, hi = groups[g]
        for j in range(lo, hi):
            dispatch[c, j].wait_recv()
        some = blocks(lo, hi)
        pair_send(2 + 2 * g, c, rows.at[c, 0, some], rows.at[c, 2, some], chip)
        pair_send(3 + 2 * g, c, rows.at[c, 0, some], rows.at[c, 1, some], core)

    def relay(c):
        for kind in (0, 2, 4, 6):
            links[kind, c].wait_recv()
        pair_send(8, c, rows.at[c, 2], rows.at[c, 3], core)

    def pieces(c):
        return LAST_PIECES if c == chunks - 1 else 1

    def columns(c, q):
        size = part.shape[3] // pieces(c)
        return pl.ds(q * size, size)

    def part_send(kind, c, q, src, dst, peer):
        links[kind, c, q] = remote(
            src, dst, part_go.at[kind, c, q], part_come.at[kind, c, q], peer
        )

    def compute(c):
        e = c // per_expert
        if c == 0:
            for copy in w_copies:
                copy.wait()
        own_copies[c].wait()
        for kind in (1, 3, 5, 7, 8):
            links[kind, c].wait_recv()
        block = rows.shape[2]

        def project_in(t, carry):
            cols = pl.ds(pl.multiple_of(t * TILE, TILE), TILE)
            x = rows[c].reshape(4 * block, rows.shape[3])
            h = exact_dot(x, first[e, :, cols])
            hidden[:, cols] = jnp.maximum(h, 0.0).astype(jnp.bfloat16)
            return carry

        lax.fori_loop(0, first.shape[2] // TILE, project_in, 0)

        def project_out(t, carry):
            cols = pl.ds(pl.multiple_of(t * TILE, TILE), TILE)
            y = exact_dot(hidden[...], second[e, :, cols]).astype(jnp.bfloat16)
            for k in range(4):
                part[c, k, :, cols] = y[k * block : (k + 1) * block]
            return carry

        steps = second.shape[2] // TILE // pieces(c)
        for q in range(pieces(c)):
            lax.fori_loop(q * steps, (q + 1) * steps, project_out, 0)
            cols = columns(c, q)
            part_send(0, c, q, part.at[c, 3, :, cols], near.at[c, 1, :, cols], core)
            part_send(1, c, q, part.at[c, 1, :, cols], near.at[c, 0, :, cols], core)

    def over_rows(body):
        def step(t, carry):
            body(pl.ds(pl.multiple_of(t * ROWS, ROWS), ROWS))
            return carry

        lax.fori_loop(0, n, step, 0)

    def wide(x):
        return x.astype(jnp.float32)

    def cross(c):
        for q in range(pieces(c)):
            links[0, c, q].wait_recv()
            cols = columns(c, q)

            def add(r):
                both = wide(part[c, 2, r, cols]) + wide(near[c, 1, r, cols])
                part[c, 2, r, cols] = both.astype(jnp.bfloat16)

            over_rows(add)
            part_send(2, c, q, part.at[c, 2, :, cols], far.at[c, :, cols], chip)

    def finish(c):
        for q in range(pieces(c)):
            links[1, c, q].wait_recv()
            links[2, c, q].wait_recv()
            cols = columns(c, q)

            def add(r):
                both = wide(part[c, 0, r, cols]) + wide(near[c, 0, r, cols])
                both = both + wide(far[c, r, cols])
                part[c, 0, r, cols] = both.astype(jnp.bfloat16)

            over_rows(add)
            for j in range(1, n):
                some = blocks(j, j + 1)
                sent.append(
                    remote(
                        part.at[c, 0, some, cols],
                        back.at[c, some, cols],
                        ret_go.at[c, q, j],
                        ret_come.at[c, q, j],
                        ahead[j],
                    )
                )
            own = blocks(0, 1)
            copy = pltpu.make_async_copy(
                part.at[c, 0, own, cols], back.at[c, own, cols], ret_own.at[c, q]
            )
            copy.start()
            sent.append(copy)

    def spread0(c):
        spread(c, 1)

    def spread1(c):
        spread(c, 2)

    for c in range(chunks):
        spread(c, 0)

    order = [(spread0, 0), (relay, 1), (spread1, 0), (compute, 1), (cross, 1), (finish, 2)]
    for i in range(chunks + 3):
        for stage, late in order:
            if 0 <= i - late < chunks:
                stage(i - late)

    for copy in dispatch.values():
        copy.wait_send()
    for copy in links.values():
        copy.wait_send()
    for copy in sent:
        copy.wait()


def look_up(table, ids):
    lines = table.reshape(-1, LANES).astype(jnp.bfloat16)
    line = ids[:, None] // LANES == jnp.arange(lines.shape[0], dtype=jnp.int32)[None, :]
    found = exact_dot(line.astype(jnp.bfloat16), lines)
    lane = ids[:, None] % LANES == jnp.arange(LANES, dtype=jnp.int32)[None, :]
    return jnp.sum(jnp.where(lane, found, 0.0), axis=1).astype(jnp.int32)


def expert_layer(packed, w_in, w_out, n):
    chunks, block, width = packed.shape
    quarter = w_in.shape[2]
    bf16 = jnp.bfloat16
    dma = pltpu.SemaphoreType.DMA
    anywhere = pl.BlockSpec(memory_space=pl.ANY)
    return pl.pallas_call(
        functools.partial(layer_kernel, n),
        out_shape=jax.ShapeDtypeStruct(packed.shape, bf16),
        in_specs=[anywhere] * 3,
        out_specs=anywhere,
        scratch_shapes=[
            pltpu.VMEM(w_in.shape, bf16),
            pltpu.VMEM(w_out.shape, bf16),
            pltpu.VMEM((chunks, 4, block, width), bf16),
            pltpu.VMEM((4 * block, quarter), bf16),
            pltpu.VMEM((chunks, 4, block, width), bf16),
            pltpu.VMEM((chunks, 2, block, width), bf16),
            pltpu.VMEM((chunks, block, width), bf16),
            dma((chunks,)),
            dma((2,)),
            dma((chunks, n)),
            dma((chunks, n)),
            dma((9, chunks)),
            dma((9, chunks)),
            dma((3, chunks, LAST_PIECES)),
            dma((3, chunks, LAST_PIECES)),
            dma((chunks, LAST_PIECES, n)),
            dma((chunks, LAST_PIECES, n)),
            dma((chunks, LAST_PIECES)),
        ],
        compiler_params=pltpu.CompilerParams(
            collective_id=0, has_side_effects=True, vmem_limit_bytes=60 * 1024 * 1024
        ),
    )(packed, w_in, w_out)


def plain(tokens, token_ids, table, w_in, w_out):
    groups = lax.axis_size("expert")
    exp_local = w_in.shape[0]
    experts = groups * exp_local
    tok_rows, width = tokens.shape
    slots = max(2, 2 * tok_rows // experts)
    quarter = w_out.shape[1]
    chosen = jnp.take(table, token_ids, axis=0)
    expert_hot = (chosen[:, None] == jnp.arange(experts, dtype=jnp.int32)[None, :]).astype(
        jnp.int32
    )
    earlier = jnp.cumsum(expert_hot, axis=0) - expert_hot
    rank_tok = jnp.sum(earlier * expert_hot, axis=1)
    kept = rank_tok < slots
    column = (chosen // exp_local * slots + rank_tok) * exp_local + chosen % exp_local
    placer = (
        (column[:, None] == jnp.arange(experts * slots, dtype=jnp.int32)[None, :]) & kept[:, None]
    ).astype(jnp.bfloat16)
    packed = jnp.einsum("ts,td->sd", placer, tokens, preferred_element_type=jnp.float32).astype(
        jnp.bfloat16
    )
    packed = packed.reshape(groups * slots, exp_local, width)
    arrived = lax.all_to_all(packed, "expert", split_axis=0, concat_axis=0, tiled=True)
    rows = arrived.shape[0]
    hidden = jax.nn.relu(
        jnp.einsum(
            "red,edh->reh",
            arrived,
            lax.all_gather(w_in, "pair", axis=2, tiled=True),
            preferred_element_type=jnp.float32,
        )
    ).astype(jnp.bfloat16)
    total = jnp.zeros((rows, exp_local, width), jnp.float32)
    piece = lax.all_gather(w_out, "pair", axis=1, tiled=True)
    for index in range(piece.shape[1] // quarter):
        cols = lax.dynamic_slice_in_dim(hidden, index * quarter, quarter, 2)
        part = jnp.einsum(
            "reh,ehd->red",
            cols,
            piece[:, index * quarter : (index + 1) * quarter],
            preferred_element_type=jnp.float32,
        ).astype(jnp.bfloat16)
        total = total + lax.optimization_barrier(part).astype(jnp.float32)
    result = total.astype(jnp.bfloat16)
    returned = lax.all_to_all(result, "expert", split_axis=0, concat_axis=0, tiled=True)
    flat = returned.reshape(experts * slots, width)
    return jnp.dot(placer, flat, preferred_element_type=jnp.float32).astype(jnp.bfloat16)


def on_device(tokens, token_ids, table, w_in, w_out):
    n = lax.axis_size("expert")
    me = lax.axis_index("expert")
    exp_local = w_in.shape[0]
    experts = n * exp_local
    tok_rows, width = tokens.shape
    slots = max(2, 2 * tok_rows // experts)
    if slots % ROWS or table.shape[0] % LANES or lax.axis_size("pair") != 4 or experts > 256 or n < 8 or n & (n - 1):
        return plain(tokens, token_ids, table, w_in, w_out)
    per_expert = slots // ROWS

    chosen = look_up(table, token_ids)
    hot = chosen[:, None] == jnp.arange(experts, dtype=jnp.int32)[None, :]
    before = jnp.arange(tok_rows)[:, None] > jnp.arange(tok_rows)[None, :]
    earlier = exact_dot(before.astype(jnp.bfloat16), hot.astype(jnp.bfloat16))
    rank = jnp.sum(jnp.where(hot, earlier, 0.0), axis=1).astype(jnp.int32)
    ahead = jnp.bitwise_xor(chosen // exp_local, me)
    chunk = chosen % exp_local * per_expert + rank // ROWS
    column = jnp.where(rank < slots, (chunk * n + ahead) * ROWS + rank % ROWS, -1)

    places = jnp.arange(experts * slots, dtype=jnp.int32)
    placer = (places[:, None] == column[None, :]).astype(jnp.bfloat16)
    packed = exact_dot(placer, tokens).astype(jnp.bfloat16)
    packed = packed.reshape(exp_local * per_expert, n * ROWS, width)
    back = expert_layer(packed, w_in, w_out, n).reshape(experts * slots, width)
    picker = (column[:, None] == places[None, :]).astype(jnp.bfloat16)
    return exact_dot(picker, back).astype(jnp.bfloat16)


def solution(mesh):
    in_specs = (
        P(("expert", "pair"), None),
        P(("expert", "pair")),
        P(),
        P("expert", None, "pair"),
        P("expert", "pair", None),
    )
    out_specs = P(("expert", "pair"), None)
    return jax.shard_map(
        on_device, mesh=mesh, in_specs=in_specs, out_specs=out_specs, check_vma=False
    )
```
